256 devices in a mesh: row: 8 (over y, core), col: 32 (over x, z).
Axes of the slice: x: 4, y: 4, z: 8, core: 2. Of those that a mesh axis runs over, the one named last changes fastest.
Arguments:
- residual: bfloat16 [2048, 32768], P('row', 'col'), may hold values from -6 to 6
- strip_weights: bfloat16 [2048, 512], P('row'), may hold values from -0.375 to 0.375
- bin_weights: bfloat16 [8, 32768, 4096], P('row', 'col'), may hold values from -0.375 to 0.375
- touched: int32 [8, 32, 32], P('row', 'col'), may hold values 0 or 1
- image: float32 [4096, 4096], P('row', 'col'), may hold values from -6 to 6
- precond: float32 [4096, 4096], P('row', 'col'), may hold values from 0.05 to 1.35, as said below
Outputs:
- updated: float32 [4096, 4096], P('row', 'col')
- mean_change: float32 [], replicated
The draws below stay inside these ranges and needn't reach their ends.
Inputs may be any that keep to these rules, and one draw needn't show every extreme that they name: `precond`: positive.
All inputs are finite; a program needn't handle non-finite values. No bound on the sum of `touched` on one device may be relied on, other than what follows from the above.
Results may differ from the reference program's by a relative error of at most 0.0023.
Values sent between devices are 32-bit elements; how exact they have to be, the bound alone decides.
No kernel may reach another device: no remote copies, remote signals or barrier semaphores. Data moves between devices by JAX's collectives and lax.ppermute only.
A program may use at most 64 MiB of HBM per device.

```python
import jax
import jax.numpy as jnp
from jax import lax

TILE_R = 512
TILE_C = 128
ANG = 256
DB = 1024
ITERS = 10
IMAGE_R = 4096
IMAGE_C = 4096
N_ROW = 8
N_COL = 32


def draw_precond(key, part):
    row_pos = lax.broadcasted_iota(jnp.float32, (IMAGE_R, IMAGE_C), 0) / (IMAGE_R - 1)
    col_pos = lax.broadcasted_iota(jnp.float32, (IMAGE_R, IMAGE_C), 1) / (IMAGE_C - 1)
    uniform_part = jax.random.uniform(key, (IMAGE_R, IMAGE_C), jnp.float32)
    base = 0.05 * jnp.exp(uniform_part * jnp.log(3.0))
    ramp = (1.0 + 2.0 * row_pos) * (1.0 + 2.0 * col_pos)
    return (base * ramp).astype(jnp.float32)


def with_ends(values, rng, low, high):
    longest = values.shape.index(max(values.shape))
    spots = []
    for shift in (0, 1):
        where = [jax.random.randint(jax.random.fold_in(rng, axis), (), 0, length) for axis, length in enumerate(values.shape)]
        where[longest] = (where[longest] + shift) % values.shape[longest]
        spots.append(tuple(where))
    return values.at[spots[0]].set(low).at[spots[1]].set(high)


def spiked(values, rng, source, target, shards_of, factor):
    def block_of(axis_at):
        return (jnp.arange(values.shape[axis_at]) // (values.shape[axis_at] // shards_of)).reshape((-1,) + (1,) * (values.ndim - 1 - axis_at))

    near = jax.random.permutation(rng, shards_of)[block_of(target)]
    second = (block_of(target) + shards_of // 2) % shards_of
    return jnp.where((block_of(source) == near) | (block_of(source) == second), factor * values, values)


def level_of(rng, extent, cuts, low, high):
    def one(dim, blocks):
        draws = jax.random.uniform(jax.random.fold_in(jax.random.fold_in(rng, 6), dim), (blocks,), jnp.float32, low / len(cuts), high / len(cuts))
        return jnp.repeat(jnp.exp(draws), extent[dim] // blocks).reshape((-1,) + (1,) * (len(extent) - dim - 1))

    gain = one(*cuts[0])
    for cut in cuts[1:]:
        gain = gain * one(*cut)
    return gain


def scatter_about(own_key, dims, deviation, most, split=(), held_as=jnp.bfloat16):
    values = jax.random.normal(own_key, dims, jnp.float32) * deviation
    if len(split) > 0:
        values = level_of(own_key, dims, split, -0.22, 0.18) * values
    return jnp.clip(values, min=-most, max=most).astype(held_as)


def noise_with(stream_key, dims, deviation, bound, split, heavy, kind=jnp.bfloat16):
    values = deviation * jax.random.normal(stream_key, dims, jnp.float32)
    if split:
        values = values * level_of(stream_key, dims, split, -0.22, 0.18)
    return jnp.clip(spiked(values, jax.random.fold_in(stream_key, 3), *heavy), -bound, bound).astype(kind)


def setup_inputs(seed: int = 0) -> dict:
    streams_of = jax.random.split(jax.random.key(seed), 7)
    residual = scatter_about(streams_of[0], (N_ROW * ANG, N_COL * DB), 1.0, 6.0, ((0, 8), (1, 32)))
    strip_weights = scatter_about(streams_of[1], (N_ROW * ANG, TILE_R), ANG ** -0.5, 0.375, ((0, 8),))
    bin_weights = noise_with(streams_of[2], (N_ROW, N_COL * DB, IMAGE_C), DB ** -0.5, 0.375, ((0, 8), (1, 32)), (1, 2, 32, 2.75))
    touched = with_ends((jax.random.randint(streams_of[3], (N_ROW, N_COL, N_COL), 0, 4) < 3).astype(jnp.int32), jax.random.fold_in(streams_of[3], 1), 0, 1)
    image = scatter_about(streams_of[4], (IMAGE_R, IMAGE_C), 1.0, 6.0, ((0, 8), (1, 32)), jnp.float32)
    precond = draw_precond(jax.random.fold_in(streams_of[6], 71), 0)
    return {"residual": residual, "strip_weights": strip_weights, "bin_weights": bin_weights, "touched": touched, "image": image, "precond": precond}


tv_weight = 0.25
dual_step = 0.125
radius = 0.25
epsilon = 1e-06

def divergence(down, right):
    above = jnp.concatenate([jnp.zeros_like(down[:1]), down[:-1]], 0)
    beside = jnp.concatenate([jnp.zeros_like(right[:, :1]), right[:, :-1]], 1)
    return down - above + (right - beside)

def reference(residual, strip_weights, bin_weights, touched, image, precond):
    strips = []
    for strip_index in range(N_ROW):
        sinogram = residual[strip_index * ANG:(strip_index + 1) * ANG]
        sinogram = jnp.transpose(sinogram.reshape(ANG, N_COL, DB), (1, 0, 2))
        weights = bin_weights[strip_index].reshape(N_COL, DB, IMAGE_C)
        marks = touched[strip_index].astype(jnp.float32)

        def add_block(running, pieces):
            sino_block, weight_block, tile_marks = pieces
            product = jnp.dot(sino_block, weight_block, preferred_element_type=jnp.float32)
            product = product.reshape(ANG, N_COL, TILE_C) * tile_marks[None, :, None]
            return (running + product, None)
        summed, _unused = lax.scan(add_block, jnp.zeros((ANG, N_COL, TILE_C), jnp.float32), (sinogram, weights, marks))
        factor_block = strip_weights[strip_index * ANG:(strip_index + 1) * ANG].astype(jnp.float32)
        strip = jnp.einsum('ar,act->rct', factor_block, summed, precision=lax.Precision.HIGHEST)
        strips.append(strip.reshape(TILE_R, IMAGE_C))
    gradient = jnp.concatenate(strips, 0)
    step_dir = precond * gradient
    spread = jnp.sqrt(jnp.sum(step_dir * step_dir) / (IMAGE_R * IMAGE_C) + epsilon)
    factor = jnp.minimum(1.0, radius / spread)
    source = image - factor * step_dir
    scaled = source / tv_weight
    down = jnp.zeros_like(source)
    right = jnp.zeros_like(source)
    for turn_index in range(ITERS):
        potential = divergence(down, right) - scaled
        grad_down = jnp.concatenate([potential[1:] - potential[:-1], jnp.zeros_like(potential[:1])], 0)
        grad_right = jnp.concatenate([potential[:, 1:] - potential[:, :-1], jnp.zeros_like(potential[:, :1])], 1)
        magnitude = jnp.sqrt(grad_down * grad_down + grad_right * grad_right)
        divisor = 1.0 + dual_step * magnitude
        down = (down + dual_step * grad_down) / divisor
        right = (right + dual_step * grad_right) / divisor
    updated = source - tv_weight * divergence(down, right)
    change = updated - image
    mean_change = jnp.sum(change * change) / (IMAGE_R * IMAGE_C)
    return (updated, mean_change)
```

```python
import functools

import jax
import jax.numpy as jnp
from jax import lax
from jax.experimental import pallas as pl
from jax.experimental.pallas import tpu as pltpu
from jax.sharding import Mesh
from jax.sharding import PartitionSpec as P

ITERS = 10
COL = ("col_0", "col_1")
ROW = ("row_0", "row_1")
ROW_COL = ("row_0", "row_1", "col_0", "col_1")

tv_weight = 0.25
dual_step = 0.125
radius = 0.25
epsilon = 1e-06

HALO = 16
LANES = 128
BASE = 8


def vmem():
    return pl.BlockSpec(memory_space=pltpu.VMEM)


def smem():
    return pl.BlockSpec(memory_space=pltpu.SMEM)


def back_project_kernel(marks, residual, weights, out, *, tiles, per_x):
    first = (pl.program_id(0) * per_x) + pl.program_id(1) * tiles
    product = jnp.dot(residual[...], weights[...], preferred_element_type=jnp.float32)
    for k in range(tiles):
        mark = marks[0, first + k].astype(jnp.float32)
        out[k, 0] = product[:, k * LANES:(k + 1) * LANES] * mark


def back_project(residual, weights, marks, n_x, n_z):
    angles, bins = residual.shape
    tiles = 4
    return pl.pallas_call(
        functools.partial(back_project_kernel, tiles=tiles, per_x=n_z),
        grid=(n_x, n_z // tiles),
        in_specs=[
            smem(),
            pl.BlockSpec((angles, bins), lambda x, h: (0, 0)),
            pl.BlockSpec((None, bins, tiles * LANES), lambda x, h: (0, 0, x * (n_z // tiles) + h)),
        ],
        out_specs=pl.BlockSpec((tiles, 1, angles, LANES), lambda x, h: (h, x, 0, 0)),
        out_shape=jax.ShapeDtypeStruct((n_z, n_x, angles, LANES), jnp.float32),
    )(marks, residual, weights)


def exact_parts(value):
    high = value.astype(jnp.bfloat16)
    rest = value - high.astype(jnp.float32)
    middle = rest.astype(jnp.bfloat16)
    low = (rest - middle.astype(jnp.float32)).astype(jnp.bfloat16)
    return high, middle, low


def gradient_kernel(place, parts, strip, precond, step_dir, slots, *, n_row):
    summed = parts[0]
    for k in range(1, parts.shape[0]):
        summed = summed + parts[k]
    gradient = None
    for piece in reversed(exact_parts(summed)):
        term = jnp.dot(strip[...], piece, preferred_element_type=jnp.float32)
        gradient = term if gradient is None else gradient + term
    value = precond[...] * gradient
    step_dir[...] = value
    rows = value.shape[0]
    squares = value * value
    partial = squares[0:8]
    for k in range(1, rows // 8):
        partial = partial + squares[8 * k:8 * k + 8]
    own = place[0]
    initial = value[0:HALO]
    last = value[rows - HALO:rows]
    for k in range(n_row):
        slots[k, 0:HALO] = jnp.where(own < k, last, initial)
        slots[k, HALO:HALO + 8] = partial


def make_gradient(place, parts, strip, precond, n_row):
    rows = strip.shape[0]
    return pl.pallas_call(
        functools.partial(gradient_kernel, n_row=n_row),
        in_specs=[smem(), vmem(), vmem(), vmem()],
        out_specs=[vmem(), vmem()],
        out_shape=[
            jax.ShapeDtypeStruct((rows, LANES), jnp.float32),
            jax.ShapeDtypeStruct((n_row, HALO + 8, LANES), jnp.float32),
        ],
    )(place, parts, strip, precond)


def edges_kernel(place, received, step_dir, leftward, rightward, slots, padded, *, n_row):
    own = place[0]
    rows = step_dir.shape[0]
    padded[0:HALO] = received[jnp.maximum(own - 1, 0), 0:HALO]
    padded[HALO:HALO + rows] = step_dir[...]
    padded[HALO + rows:rows + 2 * HALO] = received[jnp.minimum(own + 1, n_row - 1), 0:HALO]
    padded[rows + 2 * HALO:] = jnp.zeros((padded.shape[0] - rows - 2 * HALO, LANES), jnp.float32)
    for k in range(padded.shape[0] // LANES):
        block = padded[k * LANES:(k + 1) * LANES].T
        leftward[:, k * LANES:(k + 1) * LANES] = block[0:HALO]
        rightward[:, k * LANES:(k + 1) * LANES] = block[LANES - HALO:]
    partial = received[0, HALO:HALO + 8]
    for k in range(1, n_row):
        partial = partial + received[k, HALO:HALO + 8]
    total = jnp.sum(partial, axis=0, keepdims=True)
    slots[...] = jnp.broadcast_to(total[None], slots.shape)


def make_edges(place, received, step_dir, n_row, n_col):
    rows = step_dir.shape[0]
    length = -(-(rows + 2 * HALO) // LANES) * LANES
    edge = jax.ShapeDtypeStruct((HALO, length), jnp.float32)
    return pl.pallas_call(
        functools.partial(edges_kernel, n_row=n_row),
        in_specs=[smem(), vmem(), vmem()],
        out_specs=[vmem(), vmem(), vmem()],
        out_shape=[edge, edge, jax.ShapeDtypeStruct((n_col, 1, LANES), jnp.float32)],
        scratch_shapes=[pltpu.VMEM((length, LANES), jnp.float32)],
    )(place, received, step_dir)


def denoise_kernel(
    place, sums, received, step_dir, from_right, from_left, image_main, image_side,
    updated, slots, scaled, down, right, potential, down_mask, right_mask,
    *, n_row, n_col,
):
    own_row, own_col = place[0], place[1]
    rows = step_dir.shape[0]
    band = rows + 2 * HALO
    cells = float(n_row * rows * n_col * LANES)
    square_sum = jnp.sum(jnp.sum(sums[...], axis=0), axis=1, keepdims=True)
    spread = jnp.sqrt(square_sum / cells + epsilon)
    factor = jnp.minimum(1.0, radius / spread)

    zero = jnp.zeros((2, 8, LANES), jnp.float32)
    for plane in (scaled, down, right, potential):
        plane[:, 0:BASE] = zero
        plane[:, BASE + band:BASE + band + 8] = zero

    lane = lax.broadcasted_iota(jnp.int32, (8, LANES), 1)
    sub = lax.broadcasted_iota(jnp.int32, (8, LANES), 0)
    first_lane = lane == 0
    last_lane = lane == LANES - 1
    total_rows = n_row * rows
    total_cols = n_col * LANES
    columns = (
        own_col * LANES + lane,
        own_col * LANES + lane + jnp.where(lane < LANES // 2, LANES, -LANES),
    )
    column_in = [(c >= 0) & (c < total_cols) for c in columns]
    column_not_last = [(c >= 0) & (c < total_cols - 1) for c in columns]
    for at in range(BASE, BASE + band, 8):
        row = own_row * rows + (at - BASE - HALO) + sub
        row_in = (row >= 0) & (row < total_rows)
        row_not_last = (row >= 0) & (row < total_rows - 1)
        for t in range(2):
            down_mask[t, at:at + 8] = jnp.where(row_not_last & column_in[t], dual_step, 0.0)
            right_mask[t, at:at + 8] = jnp.where(row_in & column_not_last[t], dual_step, 0.0)
            down[t, at:at + 8] = zero[0]
            right[t, at:at + 8] = zero[0]

    scaled[0, BASE:BASE + HALO] = received[jnp.maximum(own_row - 1, 0), 0:HALO]
    scaled[0, BASE + HALO + rows:BASE + band] = received[jnp.minimum(own_row + 1, n_row - 1), 0:HALO]
    gap = jnp.zeros((LANES - 2 * HALO, LANES), jnp.float32)
    for k in range(from_right.shape[1] // LANES):
        here = slice(k * LANES, (k + 1) * LANES)
        block = jnp.concatenate([from_right[:, here], gap, from_left[:, here]], axis=0).T
        count = min(LANES, band - k * LANES)
        scaled[1, BASE + k * LANES:BASE + k * LANES + count] = block[0:count]
    for at in range(BASE, BASE + band, 8):
        from_tile = BASE + HALO <= at < BASE + HALO + rows
        direction = step_dir[at - BASE - HALO:at - BASE - HALO + 8] if from_tile else scaled[0, at:at + 8]
        scaled[0, at:at + 8] = (image_main[at - BASE:at - BASE + 8] - factor * direction) / tv_weight
        scaled[1, at:at + 8] = (image_side[at - BASE:at - BASE + 8] - factor * scaled[1, at:at + 8]) / tv_weight

    def right_divergence(at, t):
        mine = right[t, at:at + 8]
        rolled = pltpu.roll(mine, 1, 1)
        across = pltpu.roll(right[1 - t, at:at + 8], 1, 1)
        return mine - jnp.where(first_lane, across, rolled)

    def turn(_, carry):
        for at in range(BASE, BASE + band, 8):
            rolled = [pltpu.roll(right[t, at:at + 8], 1, 1) for t in range(2)]
            for t in range(2):
                beside = jnp.where(first_lane, rolled[1 - t], rolled[t])
                potential[t, at:at + 8] = (
                    (down[t, at:at + 8] - down[t, at - 1:at + 7])
                    + (right[t, at:at + 8] - beside)
                    - scaled[t, at:at + 8]
                )
        for at in range(BASE, BASE + band, 8):
            here = [potential[t, at:at + 8] for t in range(2)]
            rolled = [pltpu.roll(here[t], LANES - 1, 1) for t in range(2)]
            for t in range(2):
                beside = jnp.where(last_lane, rolled[1 - t], rolled[t])
                step_down = (potential[t, at + 1:at + 9] - here[t]) * down_mask[t, at:at + 8]
                step_right = (beside - here[t]) * right_mask[t, at:at + 8]
                square = step_down * step_down + step_right * step_right
                size = square * lax.rsqrt(jnp.maximum(square, 1e-36))
                inverse = 1.0 / (1.0 + size)
                down[t, at:at + 8] = (down[t, at:at + 8] + step_down) * inverse
                right[t, at:at + 8] = (right[t, at:at + 8] + step_right) * inverse
        return carry

    lax.fori_loop(0, ITERS, turn, 0)

    change_sum = jnp.zeros((8, LANES), jnp.float32)
    for at in range(BASE + HALO, BASE + HALO + rows, 8):
        inner = at - BASE - HALO
        picture = image_main[at - BASE:at - BASE + 8]
        source = picture - factor * step_dir[inner:inner + 8]
        divergence = (down[0, at:at + 8] - down[0, at - 1:at + 7]) + right_divergence(at, 0)
        result = source - tv_weight * divergence
        updated[inner:inner + 8] = result
        change = result - picture
        change_sum = change_sum + change * change
    total = jnp.sum(change_sum, axis=0, keepdims=True)
    slots[...] = jnp.broadcast_to(total[None], slots.shape)


def denoise(place, sums, received, step_dir, from_right, from_left, image_main, image_side, n_row, n_col):
    rows = step_dir.shape[0]
    plane = pltpu.VMEM((2, BASE + rows + 2 * HALO + 8, LANES), jnp.float32)
    return pl.pallas_call(
        functools.partial(denoise_kernel, n_row=n_row, n_col=n_col),
        in_specs=[smem()] + [vmem()] * 7,
        out_specs=[vmem(), vmem()],
        out_shape=[
            jax.ShapeDtypeStruct((rows, LANES), jnp.float32),
            jax.ShapeDtypeStruct((n_row * n_col, 1, LANES), jnp.float32),
        ],
        scratch_shapes=[plane] * 6,
    )(place, sums, received, step_dir, from_right, from_left, image_main, image_side)


def neighbours(count):
    forward = [(i, i + 1) for i in range(count - 1)]
    return forward, [(j, i) for i, j in forward]


def image_bands(image, n_row, n_col):
    later, earlier = neighbours(n_row)
    above = lax.ppermute(image[-HALO:], ROW, later)
    below = lax.ppermute(image[:HALO], ROW, earlier)
    main = jnp.concatenate([above, image, below], axis=0)
    later, earlier = neighbours(n_col)
    left = lax.ppermute(main[:, -HALO:], COL, later)
    right = lax.ppermute(main[:, :HALO], COL, earlier)
    gap = jnp.zeros((main.shape[0], LANES - 2 * HALO), jnp.float32)
    return main, jnp.concatenate([right, gap, left], axis=1)


def local(residual, strip_weights, bin_weights, touched, image, precond):
    n_row = lax.axis_size(ROW)
    n_col = lax.axis_size(COL)
    n_x = lax.axis_size("col_0")
    n_z = lax.axis_size("col_1")
    place = jnp.stack([lax.axis_index(ROW), lax.axis_index(COL)]).astype(jnp.int32)
    angles = residual.shape[0]
    product = back_project(residual, bin_weights, touched[0], n_x, n_z)
    product, image, strip_weights = lax.optimization_barrier((product, image, strip_weights))
    by_z = lax.psum_scatter(
        product.reshape(n_z * n_x, angles, LANES), "col_1", scatter_dimension=0, tiled=True
    )
    image_main, image_side = image_bands(image, n_row, n_col)
    strip = strip_weights.T
    parts = lax.all_to_all(by_z, "col_0", 0, 0, tiled=True)
    step_dir, row_slots = make_gradient(place, parts, strip, precond, n_row)
    received = lax.all_to_all(row_slots, ROW, 0, 0, tiled=True)
    leftward, rightward, sum_slots = make_edges(place, received, step_dir, n_row, n_col)
    later, earlier = neighbours(n_col)
    from_right = lax.ppermute(leftward, COL, earlier)
    from_left = lax.ppermute(rightward, COL, later)
    sums = lax.all_to_all(sum_slots, COL, 0, 0, tiled=True)
    updated, change_slots = denoise(
        place, sums, received, step_dir, from_right, from_left, image_main, image_side, n_row, n_col
    )
    changes = lax.all_to_all(change_slots, ROW_COL, 0, 0, tiled=True)
    cells = float(n_row * image.shape[0] * n_col * image.shape[1])
    return updated, jnp.sum(changes) / cells


def solution(mesh):
    split = Mesh(mesh.devices.reshape(4, 2, 4, 8), ("row_0", "row_1", "col_0", "col_1"))
    placed = (
        P(ROW, COL),
        P(ROW, None),
        P(ROW, COL, None),
        P(ROW, COL, None),
        P(ROW, COL),
        P(ROW, COL),
    )
    return jax.shard_map(
        local, mesh=split, in_specs=placed, out_specs=(P(ROW, COL), P()), check_vma=False
    )
```

```python
import functools

import jax
import jax.numpy as jnp
from jax import lax
from jax.experimental import pallas as pl
from jax.experimental.pallas import tpu as pltpu
from jax.sharding import Mesh
from jax.sharding import PartitionSpec as P


ITERS = 10
COL = ("col_0", "col_1")
ROW = ("row_0", "row_1")
ROW_COL = ("row_0", "row_1", "col_0", "col_1")

tv_weight = 0.25
dual_step = 0.125
radius = 0.25
epsilon = 1e-06

HALO = 16
FIRST = 96
LANES = 128
BASE = 8


def vmem():
    return pl.BlockSpec(memory_space=pltpu.VMEM)


def smem():
    return pl.BlockSpec(memory_space=pltpu.SMEM)


def params(mebibytes):
    return pltpu.CompilerParams(vmem_limit_bytes=mebibytes * 1024 * 1024)


def back_project_kernel(marks, residual, weights, *outs, plan, splits, width, n_x, n_z):
    own = lax.axis_index("col_0")
    for o, (step, low, high) in enumerate(plan):
        x = lax.rem(own + step, n_x)
        for z in range(low, high, width):
            tile = x * n_z + z
            columns = pl.ds(pl.multiple_of(tile * LANES, width * LANES), width * LANES)
            product = jnp.dot(
                residual[...], weights[0, :, columns], preferred_element_type=jnp.float32
            )
            for t in range(width):
                mark = marks[0, tile + t].astype(jnp.float32)
                marked = product[:, t * LANES:(t + 1) * LANES] * mark
                for s, (first, last) in enumerate(splits):
                    outs[o * len(splits) + s][z - low + t] = marked[first:last]


def back_project(residual, weights, marks, plan, splits, n_x, n_z):
    outs = pl.pallas_call(
        functools.partial(
            back_project_kernel, plan=plan, splits=splits, width=4, n_x=n_x, n_z=n_z
        ),
        in_specs=[smem(), vmem(), vmem()],
        out_specs=[vmem()] * (len(plan) * len(splits)),
        out_shape=[
            jax.ShapeDtypeStruct((high - low, last - first, LANES), jnp.float32)
            for _, low, high in plan for first, last in splits
        ],
        compiler_params=params(32),
    )(marks, residual, weights)
    return [outs[i:i + len(splits)] for i in range(0, len(outs), len(splits))]


def relay_kernel(ahead, behind, from_behind, from_ahead, to_ahead, to_behind):
    half = ahead.shape[0] // 2
    for k in range(half):
        to_ahead[k] = ahead[k] + from_behind[k]
        to_ahead[half + k] = ahead[half + k]
        to_behind[k] = behind[k]
        to_behind[half + k] = behind[half + k] + from_ahead[k]


def relay(ahead, behind, from_behind, from_ahead):
    shape = jax.ShapeDtypeStruct(ahead.shape, jnp.float32)
    return pl.pallas_call(
        relay_kernel,
        in_specs=[vmem()] * 4,
        out_specs=[vmem()] * 2,
        out_shape=[shape, shape],
        compiler_params=params(8),
    )(ahead, behind, from_behind, from_ahead)


def add_up_kernel(*refs):
    *parts, out = refs
    total = parts[0][...]
    for part in parts[1:]:
        total = total + part[...]
    out[...] = total


def add_up(*parts):
    return pl.pallas_call(
        add_up_kernel,
        in_specs=[vmem()] * len(parts),
        out_specs=vmem(),
        out_shape=jax.ShapeDtypeStruct(parts[0].shape, jnp.float32),
        compiler_params=params(8),
    )(*parts)


def exact_parts(value):
    high = value.astype(jnp.bfloat16)
    rest = value - high.astype(jnp.float32)
    middle = rest.astype(jnp.bfloat16)
    low = (rest - middle.astype(jnp.float32)).astype(jnp.bfloat16)
    return high, middle, low


def gradient_kernel(*refs, n_row):
    *groups, strip, precond, image, step_dir, slots = refs
    sums = []
    for parts in groups:
        total = parts[0]
        for k in range(1, parts.shape[0]):
            total = total + parts[k]
        sums.append(total)
    summed = jnp.concatenate(sums, axis=0)
    gradient = None
    for piece in reversed(exact_parts(summed)):
        term = jnp.dot(strip[...], piece, preferred_element_type=jnp.float32)
        gradient = term if gradient is None else gradient + term
    value = precond[...] * gradient
    step_dir[...] = value
    rows = value.shape[0]
    squares = value * value
    partial = squares[0:8]
    for k in range(1, rows // 8):
        partial = partial + squares[8 * k:8 * k + 8]
    own = lax.axis_index(ROW)
    last = slice(rows - HALO, rows)
    for k in range(n_row):
        below = own < k
        slots[k, 0:HALO] = jnp.where(below, value[last], value[0:HALO])
        slots[k, HALO:2 * HALO] = jnp.where(below, image[last], image[0:HALO])
        slots[k, 2 * HALO:2 * HALO + 8] = partial


def make_gradient(groups, strip, precond, image, n_row):
    rows = strip.shape[0]
    return pl.pallas_call(
        functools.partial(gradient_kernel, n_row=n_row),
        in_specs=[vmem()] * (len(groups) + 3),
        out_specs=[vmem(), vmem()],
        out_shape=[
            jax.ShapeDtypeStruct((rows, LANES), jnp.float32),
            jax.ShapeDtypeStruct((n_row, 2 * HALO + 8, LANES), jnp.float32),
        ],
        compiler_params=params(8),
    )(*groups, strip, precond, image)


def edges_kernel(received, step_dir, image, leftward, rightward, slots, padded, *, n_row):
    own = lax.axis_index(ROW)
    rows = step_dir.shape[0]
    above = jnp.maximum(own - 1, 0)
    below = jnp.minimum(own + 1, n_row - 1)
    padded[rows + 2 * HALO:] = jnp.zeros((padded.shape[0] - rows - 2 * HALO, LANES), jnp.float32)
    for part, tile in enumerate((step_dir, image)):
        layers = slice(part * HALO, (part + 1) * HALO)
        padded[0:HALO] = received[above, layers]
        padded[HALO:HALO + rows] = tile[...]
        padded[HALO + rows:rows + 2 * HALO] = received[below, layers]
        for k in range(padded.shape[0] // LANES):
            here = slice(k * LANES, (k + 1) * LANES)
            block = padded[here].T
            leftward[layers, here] = block[0:HALO]
            rightward[layers, here] = block[LANES - HALO:]
    partial = received[0, 2 * HALO:2 * HALO + 8]
    for k in range(1, n_row):
        partial = partial + received[k, 2 * HALO:2 * HALO + 8]
    total = jnp.sum(partial, axis=0, keepdims=True)
    slots[...] = jnp.broadcast_to(total[None], slots.shape)


def make_edges(received, step_dir, image, n_row, n_col):
    rows = step_dir.shape[0]
    length = -(-(rows + 2 * HALO) // LANES) * LANES
    edge = jax.ShapeDtypeStruct((2 * HALO, length), jnp.float32)
    return pl.pallas_call(
        functools.partial(edges_kernel, n_row=n_row),
        in_specs=[vmem()] * 3,
        out_specs=[vmem(), vmem(), vmem()],
        out_shape=[edge, edge, jax.ShapeDtypeStruct((n_col, 1, LANES), jnp.float32)],
        scratch_shapes=[pltpu.VMEM((length, LANES), jnp.float32)],
        compiler_params=params(4),
    )(received, step_dir, image)


def denoise_kernel(
    sums, received, step_dir, image, from_right, from_left,
    updated, slots, scaled, down, right, potential, down_mask, right_mask,
    *, n_row, n_col,
):
    own_row, own_col = lax.axis_index(ROW), lax.axis_index(COL)
    rows = step_dir.shape[0]
    band = rows + 2 * HALO
    cells = float(n_row * rows * n_col * LANES)
    square_sum = jnp.sum(jnp.sum(sums[...], axis=0), axis=1, keepdims=True)
    spread = jnp.sqrt(square_sum / cells + epsilon)
    factor = jnp.minimum(1.0, radius / spread)

    zero = jnp.zeros((2, 8, LANES), jnp.float32)
    for plane in (scaled, down, right, potential):
        plane[:, 0:BASE] = zero
        plane[:, BASE + band:BASE + band + 8] = zero

    lane = lax.broadcasted_iota(jnp.int32, (8, LANES), 1)
    sub = lax.broadcasted_iota(jnp.int32, (8, LANES), 0)
    first_lane = lane == 0
    last_lane = lane == LANES - 1
    total_rows = n_row * rows
    total_cols = n_col * LANES
    columns = (
        own_col * LANES + lane,
        own_col * LANES + lane + jnp.where(lane < LANES // 2, LANES, -LANES),
    )
    column_in = [(c >= 0) & (c < total_cols) for c in columns]
    column_not_last = [(c >= 0) & (c < total_cols - 1) for c in columns]
    for at in range(BASE, BASE + band, 8):
        row = own_row * rows + (at - BASE - HALO) + sub
        row_in = (row >= 0) & (row < total_rows)
        row_not_last = (row >= 0) & (row < total_rows - 1)
        for t in range(2):
            down_mask[t, at:at + 8] = jnp.where(row_not_last & column_in[t], dual_step, 0.0)
            right_mask[t, at:at + 8] = jnp.where(row_in & column_not_last[t], dual_step, 0.0)
            down[t, at:at + 8] = zero[0]
            right[t, at:at + 8] = zero[0]

    def scale(direction, picture):
        return (picture - factor * direction) / tv_weight

    above = jnp.maximum(own_row - 1, 0)
    below = jnp.minimum(own_row + 1, n_row - 1)
    for there, at in ((above, BASE), (below, BASE + HALO + rows)):
        for k in range(0, HALO, 8):
            scaled[0, at + k:at + k + 8] = scale(
                received[there, k:k + 8], received[there, HALO + k:HALO + k + 8]
            )
    for at in range(0, rows, 8):
        scaled[0, BASE + HALO + at:BASE + HALO + at + 8] = scale(
            step_dir[at:at + 8], image[at:at + 8]
        )
    gap = jnp.zeros((LANES - 2 * HALO, LANES), jnp.float32)
    for k in range(from_right.shape[1] // LANES):
        here = slice(k * LANES, (k + 1) * LANES)
        edges = [
            scale(edge[0:HALO, here], edge[HALO:2 * HALO, here]) for edge in (from_right, from_left)
        ]
        block = jnp.concatenate([edges[0], gap, edges[1]], axis=0).T
        count = min(LANES, band - k * LANES)
        scaled[1, BASE + k * LANES:BASE + k * LANES + count] = block[0:count]

    def right_divergence(at, t):
        mine = right[t, at:at + 8]
        rolled = pltpu.roll(mine, 1, 1)
        across = pltpu.roll(right[1 - t, at:at + 8], 1, 1)
        return mine - jnp.where(first_lane, across, rolled)

    def turn(_, carry):
        for at in range(BASE, BASE + band, 8):
            rolled = [pltpu.roll(right[t, at:at + 8], 1, 1) for t in range(2)]
            for t in range(2):
                beside = jnp.where(first_lane, rolled[1 - t], rolled[t])
                potential[t, at:at + 8] = (
                    (down[t, at:at + 8] - down[t, at - 1:at + 7])
                    + (right[t, at:at + 8] - beside)
                    - scaled[t, at:at + 8]
                )
        for at in range(BASE, BASE + band, 8):
            here = [potential[t, at:at + 8] for t in range(2)]
            rolled = [pltpu.roll(here[t], LANES - 1, 1) for t in range(2)]
            for t in range(2):
                beside = jnp.where(last_lane, rolled[1 - t], rolled[t])
                step_down = (potential[t, at + 1:at + 9] - here[t]) * down_mask[t, at:at + 8]
                step_right = (beside - here[t]) * right_mask[t, at:at + 8]
                square = step_down * step_down + step_right * step_right
                size = square * lax.rsqrt(jnp.maximum(square, 1e-36))
                inverse = 1.0 / (1.0 + size)
                down[t, at:at + 8] = (down[t, at:at + 8] + step_down) * inverse
                right[t, at:at + 8] = (right[t, at:at + 8] + step_right) * inverse
        return carry

    lax.fori_loop(0, ITERS, turn, 0)

    change_sum = jnp.zeros((8, LANES), jnp.float32)
    for at in range(BASE + HALO, BASE + HALO + rows, 8):
        inner = at - BASE - HALO
        picture = image[inner:inner + 8]
        source = picture - factor * step_dir[inner:inner + 8]
        divergence = (down[0, at:at + 8] - down[0, at - 1:at + 7]) + right_divergence(at, 0)
        result = source - tv_weight * divergence
        updated[inner:inner + 8] = result
        change = result - picture
        change_sum = change_sum + change * change
    total = jnp.sum(change_sum, axis=0, keepdims=True)
    slots[...] = jnp.broadcast_to(total[None], slots.shape)


def denoise(sums, received, step_dir, image, from_right, from_left, n_row, n_col):
    rows = step_dir.shape[0]
    plane = pltpu.VMEM((2, BASE + rows + 2 * HALO + 8, LANES), jnp.float32)
    return pl.pallas_call(
        functools.partial(denoise_kernel, n_row=n_row, n_col=n_col),
        in_specs=[vmem()] * 6,
        out_specs=[vmem(), vmem()],
        out_shape=[
            jax.ShapeDtypeStruct((rows, LANES), jnp.float32),
            jax.ShapeDtypeStruct((n_row * n_col, 1, LANES), jnp.float32),
        ],
        scratch_shapes=[plane] * 6,
        compiler_params=params(12),
    )(sums, received, step_dir, image, from_right, from_left)


def neighbours(count):
    forward = [(i, i + 1) for i in range(count - 1)]
    return forward, [(j, i) for i, j in forward]


def step(residual, strip_weights, bin_weights, touched, image, precond):
    n_row = lax.axis_size(ROW)
    n_col = lax.axis_size(COL)
    n_x = lax.axis_size("col_0")
    n_z = lax.axis_size("col_1")
    angles = residual.shape[0]
    splits = ((0, FIRST), (FIRST, angles))
    half = n_z // 2
    marks = touched[0]
    far = back_project(
        residual, bin_weights, marks, ((2, 0, half), (2, half, n_z)), splits, n_x, n_z
    )
    far, residual = lax.optimization_barrier((far, residual))
    ring = [(i, (i + 1) % n_x) for i in range(n_x)]
    back = [(j, i) for i, j in ring]

    def both_ways(forward, backward):
        return lax.ppermute(forward, "col_0", ring), lax.ppermute(backward, "col_0", back)

    relayed = [both_ways(far[0][c], far[1][c]) for c in range(2)]
    ahead, behind, own = back_project(
        residual, bin_weights, marks,
        ((1, 0, n_z), (n_x - 1, 0, n_z), (0, 0, n_z)), splits, n_x, n_z,
    )
    outgoing = [relay(ahead[c], behind[c], *relayed[c]) for c in range(2)]
    incoming = [both_ways(*outgoing[c]) for c in range(2)]
    first = add_up(own[0], *incoming[0])
    by_z = [lax.all_to_all(first, "col_1", 0, 0, tiled=True)]
    last = add_up(own[1], *incoming[1])
    last, by_z[0] = lax.optimization_barrier((last, by_z[0]))
    by_z.append(lax.all_to_all(last, "col_1", 0, 0, tiled=True))
    strip = strip_weights.T
    step_dir, row_slots = make_gradient(by_z, strip, precond, image, n_row)
    received = lax.all_to_all(row_slots, ROW, 0, 0, tiled=True)
    leftward, rightward, sum_slots = make_edges(received, step_dir, image, n_row, n_col)
    later, earlier = neighbours(n_col)
    from_right = lax.ppermute(leftward, COL, earlier)
    from_left = lax.ppermute(rightward, COL, later)
    sums = lax.all_to_all(sum_slots, COL, 0, 0, tiled=True)
    updated, change_slots = denoise(
        sums, received, step_dir, image, from_right, from_left, n_row, n_col
    )
    changes = lax.all_to_all(change_slots, ROW_COL, 0, 0, tiled=True)
    cells = float(n_row * image.shape[0] * n_col * image.shape[1])
    return updated, jnp.sum(changes) / cells


def solution(mesh):
    split = Mesh(mesh.devices.reshape(4, 2, 4, 8), ("row_0", "row_1", "col_0", "col_1"))
    placed = (
        P(ROW, COL),
        P(ROW, None),
        P(ROW, COL, None),
        P(ROW, COL, None),
        P(ROW, COL),
        P(ROW, COL),
    )
    return jax.shard_map(
        step, mesh=split, in_specs=placed, out_specs=(P(ROW, COL), P()), check_vma=False
    )
```

```python
import functools

import jax
import jax.numpy as jnp
from jax import lax
from jax.experimental import pallas as pl
from jax.experimental.pallas import tpu as pltpu
from jax.sharding import Mesh
from jax.sharding import PartitionSpec as P


ITERS = 10
COL = ("col_0", "col_1")
ROW = ("row_0", "row_1")
ROW_COL = ("row_0", "row_1", "col_0", "col_1")

tv_weight = 0.25
dual_step = 0.125
radius = 0.25
epsilon = 1e-06

HALO = 16
X_FIRST = 128
LANES = 128
BASE = 8


def vmem():
    return pl.BlockSpec(memory_space=pltpu.VMEM)


def smem():
    return pl.BlockSpec(memory_space=pltpu.SMEM)


def params(mebibytes):
    return pltpu.CompilerParams(vmem_limit_bytes=mebibytes * 1024 * 1024)


def turned(axis, steps):
    return lax.rem(lax.axis_index(axis) + steps, lax.axis_size(axis))


def marked_products(marks, residual, weights, angles, tile, width):
    columns = pl.ds(pl.multiple_of(tile * LANES, width * LANES), width * LANES)
    product = jnp.dot(
        residual[slice(*angles)], weights[0, :, columns], preferred_element_type=jnp.float32
    )
    for t in range(width):
        yield t, product[:, t * LANES:(t + 1) * LANES] * marks[0, tile + t].astype(jnp.float32)


def far_products_kernel(marks, residual, weights, x_up, x_down, z_up, z_down, *, n_x, n_z):
    split = x_up.shape[1]
    x, z = turned("col_0", n_x // 2), turned("col_1", n_z // 2)
    width = n_z // 2
    for half, out in enumerate((x_up, x_down)):
        tile = x * n_z + half * width
        for t, value in marked_products(marks, residual, weights, (0, split), tile, width):
            out[t] = value
    for half, out in enumerate((z_up, z_down)):
        for k in range(n_x // 2):
            tile = (half * (n_x // 2) + k) * n_z + z
            for _, value in marked_products(marks, residual, weights, (split, None), tile, 1):
                out[k] = value


def near_products_kernel(marks, residual, weights, by_x, by_z, *, n_x, n_z):
    split = by_x.shape[2]
    width = n_z // 2
    for step in range(n_x):
        if step == n_x // 2:
            continue
        for z in range(0, n_z, width):
            tile = turned("col_0", step) * n_z + z
            for t, value in marked_products(marks, residual, weights, (0, split), tile, width):
                by_x[step, z + t] = value
    for x in range(n_x):
        for z in range(0, n_z, width):
            tile = x * n_z + z
            for t, value in marked_products(marks, residual, weights, (split, None), tile, width):
                steps = lax.rem(z + t + n_z - lax.axis_index("col_1"), n_z)
                by_z[steps, x] = value


def back_project(kernel, residual, weights, marks, shapes, n_x, n_z):
    return pl.pallas_call(
        functools.partial(kernel, n_x=n_x, n_z=n_z),
        in_specs=[smem(), vmem(), vmem()],
        out_specs=[vmem()] * len(shapes),
        out_shape=[jax.ShapeDtypeStruct(shape + (LANES,), jnp.float32) for shape in shapes],
        compiler_params=params(32),
    )(marks, residual, weights)


def relay_kernel(chunks, from_behind, from_ahead, to_ahead, to_behind, *, step):
    ahead, behind = chunks.at[step], chunks.at[chunks.shape[0] - step]
    count = to_ahead.shape[0]
    brought = from_behind.shape[0]
    for k in range(count):
        value = ahead[k]
        to_ahead[k] = value + from_behind[k] if k < brought else value
        value = behind[k]
        here = k - (count - brought)
        to_behind[k] = value + from_ahead[here] if here >= 0 else value


def relay(chunks, from_behind, from_ahead, step):
    shape = jax.ShapeDtypeStruct(chunks.shape[1:], jnp.float32)
    return pl.pallas_call(
        functools.partial(relay_kernel, step=step),
        in_specs=[vmem()] * 3,
        out_specs=[vmem()] * 2,
        out_shape=[shape, shape],
        compiler_params=params(8),
    )(chunks, from_behind, from_ahead)


def collect_kernel(chunks, from_behind, from_ahead, up, down, out, *, axis):
    n = chunks.shape[1]
    half = up.shape[1]
    for step in range(n):
        k = turned(axis, step)
        total = chunks[0, k] + from_behind[k] + from_ahead[k]
        if step == n // 2:
            up[0], down[0] = total[:half], total[half:]
        else:
            out[step, 0], out[step, 1] = total[:half], total[half:]


def collect(chunks, from_behind, from_ahead, axis):
    _, n, angles, _ = chunks.shape
    half = jax.ShapeDtypeStruct((1, angles // 2, LANES), jnp.float32)
    return pl.pallas_call(
        functools.partial(collect_kernel, axis=axis),
        in_specs=[vmem()] * 3,
        out_specs=[vmem()] * 3,
        out_shape=[half, half, jax.ShapeDtypeStruct((n, 2, angles // 2, LANES), jnp.float32)],
        compiler_params=params(8),
    )(chunks, from_behind, from_ahead)


def exact_parts(value):
    high = value.astype(jnp.bfloat16)
    rest = value - high.astype(jnp.float32)
    middle = rest.astype(jnp.bfloat16)
    low = (rest - middle.astype(jnp.float32)).astype(jnp.bfloat16)
    return high, middle, low


def gradient_kernel(*refs, n_row):
    *groups, strip, precond, image, step_dir, slots = refs
    sums = []
    for k in range(0, len(groups), 3):
        chunks, from_behind, from_ahead = groups[k:k + 3]
        for half in range(2):
            sums.append(chunks[0, half] + from_behind[half] + from_ahead[half])
    summed = jnp.concatenate(sums, axis=0)
    gradient = None
    for piece in reversed(exact_parts(summed)):
        term = jnp.dot(strip[...], piece, preferred_element_type=jnp.float32)
        gradient = term if gradient is None else gradient + term
    value = precond[...] * gradient
    step_dir[...] = value
    rows = value.shape[0]
    squares = value * value
    partial = squares[0:8]
    for k in range(1, rows // 8):
        partial = partial + squares[8 * k:8 * k + 8]
    own = lax.axis_index(ROW)
    last = slice(rows - HALO, rows)
    for k in range(n_row):
        below = own < k
        slots[k, 0:HALO] = jnp.where(below, value[last], value[0:HALO])
        slots[k, HALO:2 * HALO] = jnp.where(below, image[last], image[0:HALO])
        slots[k, 2 * HALO:2 * HALO + 8] = partial


def make_gradient(groups, strip, precond, image, n_row):
    rows = strip.shape[0]
    return pl.pallas_call(
        functools.partial(gradient_kernel, n_row=n_row),
        in_specs=[vmem()] * (len(groups) + 3),
        out_specs=[vmem(), vmem()],
        out_shape=[
            jax.ShapeDtypeStruct((rows, LANES), jnp.float32),
            jax.ShapeDtypeStruct((n_row, 2 * HALO + 8, LANES), jnp.float32),
        ],
        compiler_params=params(8),
    )(*groups, strip, precond, image)


def edges_kernel(received, step_dir, image, leftward, rightward, slots, padded, *, n_row):
    own = lax.axis_index(ROW)
    rows = step_dir.shape[0]
    above = jnp.maximum(own - 1, 0)
    below = jnp.minimum(own + 1, n_row - 1)
    padded[rows + 2 * HALO:] = jnp.zeros((padded.shape[0] - rows - 2 * HALO, LANES), jnp.float32)
    for part, tile in enumerate((step_dir, image)):
        layers = slice(part * HALO, (part + 1) * HALO)
        padded[0:HALO] = received[above, layers]
        padded[HALO:HALO + rows] = tile[...]
        padded[HALO + rows:rows + 2 * HALO] = received[below, layers]
        for k in range(padded.shape[0] // LANES):
            here = slice(k * LANES, (k + 1) * LANES)
            block = padded[here].T
            leftward[layers, here] = block[0:HALO]
            rightward[layers, here] = block[LANES - HALO:]
    partial = received[0, 2 * HALO:2 * HALO + 8]
    for k in range(1, n_row):
        partial = partial + received[k, 2 * HALO:2 * HALO + 8]
    total = jnp.sum(partial, axis=0, keepdims=True)
    slots[...] = jnp.broadcast_to(total[None], slots.shape)


def make_edges(received, step_dir, image, n_row, n_col):
    rows = step_dir.shape[0]
    length = -(-(rows + 2 * HALO) // LANES) * LANES
    edge = jax.ShapeDtypeStruct((2 * HALO, length), jnp.float32)
    return pl.pallas_call(
        functools.partial(edges_kernel, n_row=n_row),
        in_specs=[vmem()] * 3,
        out_specs=[vmem(), vmem(), vmem()],
        out_shape=[edge, edge, jax.ShapeDtypeStruct((n_col, 1, LANES), jnp.float32)],
        scratch_shapes=[pltpu.VMEM((length, LANES), jnp.float32)],
        compiler_params=params(4),
    )(received, step_dir, image)


def denoise_kernel(
    sums, received, step_dir, image, from_right, from_left,
    updated, slots, scaled, down, right, potential, down_mask, right_mask,
    *, n_row, n_col,
):
    own_row, own_col = lax.axis_index(ROW), lax.axis_index(COL)
    rows = step_dir.shape[0]
    band = rows + 2 * HALO
    cells = float(n_row * rows * n_col * LANES)
    square_sum = jnp.sum(jnp.sum(sums[...], axis=0), axis=1, keepdims=True)
    spread = jnp.sqrt(square_sum / cells + epsilon)
    factor = jnp.minimum(1.0, radius / spread)

    zero = jnp.zeros((2, 8, LANES), jnp.float32)
    for plane in (scaled, down, right, potential):
        plane[:, 0:BASE] = zero
        plane[:, BASE + band:BASE + band + 8] = zero

    lane = lax.broadcasted_iota(jnp.int32, (8, LANES), 1)
    sub = lax.broadcasted_iota(jnp.int32, (8, LANES), 0)
    first_lane = lane == 0
    last_lane = lane == LANES - 1
    total_rows = n_row * rows
    total_cols = n_col * LANES
    columns = (
        own_col * LANES + lane,
        own_col * LANES + lane + jnp.where(lane < LANES // 2, LANES, -LANES),
    )
    column_in = [(c >= 0) & (c < total_cols) for c in columns]
    column_not_last = [(c >= 0) & (c < total_cols - 1) for c in columns]
    for at in range(BASE, BASE + band, 8):
        row = own_row * rows + (at - BASE - HALO) + sub
        row_in = (row >= 0) & (row < total_rows)
        row_not_last = (row >= 0) & (row < total_rows - 1)
        for t in range(2):
            down_mask[t, at:at + 8] = jnp.where(row_not_last & column_in[t], dual_step, 0.0)
            right_mask[t, at:at + 8] = jnp.where(row_in & column_not_last[t], dual_step, 0.0)
            down[t, at:at + 8] = zero[0]
            right[t, at:at + 8] = zero[0]

    def scale(direction, picture):
        return (picture - factor * direction) / tv_weight

    above = jnp.maximum(own_row - 1, 0)
    below = jnp.minimum(own_row + 1, n_row - 1)
    for there, at in ((above, BASE), (below, BASE + HALO + rows)):
        for k in range(0, HALO, 8):
            scaled[0, at + k:at + k + 8] = scale(
                received[there, k:k + 8], received[there, HALO + k:HALO + k + 8]
            )
    for at in range(0, rows, 8):
        scaled[0, BASE + HALO + at:BASE + HALO + at + 8] = scale(
            step_dir[at:at + 8], image[at:at + 8]
        )
    gap = jnp.zeros((LANES - 2 * HALO, LANES), jnp.float32)
    for k in range(from_right.shape[1] // LANES):
        here = slice(k * LANES, (k + 1) * LANES)
        edges = [
            scale(edge[0:HALO, here], edge[HALO:2 * HALO, here]) for edge in (from_right, from_left)
        ]
        block = jnp.concatenate([edges[0], gap, edges[1]], axis=0).T
        count = min(LANES, band - k * LANES)
        scaled[1, BASE + k * LANES:BASE + k * LANES + count] = block[0:count]

    def right_divergence(at, t):
        mine = right[t, at:at + 8]
        rolled = pltpu.roll(mine, 1, 1)
        across = pltpu.roll(right[1 - t, at:at + 8], 1, 1)
        return mine - jnp.where(first_lane, across, rolled)

    def turn(_, carry):
        for at in range(BASE, BASE + band, 8):
            rolled = [pltpu.roll(right[t, at:at + 8], 1, 1) for t in range(2)]
            for t in range(2):
                beside = jnp.where(first_lane, rolled[1 - t], rolled[t])
                potential[t, at:at + 8] = (
                    (down[t, at:at + 8] - down[t, at - 1:at + 7])
                    + (right[t, at:at + 8] - beside)
                    - scaled[t, at:at + 8]
                )
        for at in range(BASE, BASE + band, 8):
            here = [potential[t, at:at + 8] for t in range(2)]
            rolled = [pltpu.roll(here[t], LANES - 1, 1) for t in range(2)]
            for t in range(2):
                beside = jnp.where(last_lane, rolled[1 - t], rolled[t])
                step_down = (potential[t, at + 1:at + 9] - here[t]) * down_mask[t, at:at + 8]
                step_right = (beside - here[t]) * right_mask[t, at:at + 8]
                square = step_down * step_down + step_right * step_right
                size = square * lax.rsqrt(jnp.maximum(square, 1e-36))
                inverse = 1.0 / (1.0 + size)
                down[t, at:at + 8] = (down[t, at:at + 8] + step_down) * inverse
                right[t, at:at + 8] = (right[t, at:at + 8] + step_right) * inverse
        return carry

    lax.fori_loop(0, ITERS, turn, 0)

    change_sum = jnp.zeros((8, LANES), jnp.float32)
    for at in range(BASE + HALO, BASE + HALO + rows, 8):
        inner = at - BASE - HALO
        picture = image[inner:inner + 8]
        source = picture - factor * step_dir[inner:inner + 8]
        divergence = (down[0, at:at + 8] - down[0, at - 1:at + 7]) + right_divergence(at, 0)
        result = source - tv_weight * divergence
        updated[inner:inner + 8] = result
        change = result - picture
        change_sum = change_sum + change * change
    total = jnp.sum(change_sum, axis=0, keepdims=True)
    slots[...] = jnp.broadcast_to(total[None], slots.shape)


def denoise(sums, received, step_dir, image, from_right, from_left, n_row, n_col):
    rows = step_dir.shape[0]
    plane = pltpu.VMEM((2, BASE + rows + 2 * HALO + 8, LANES), jnp.float32)
    return pl.pallas_call(
        functools.partial(denoise_kernel, n_row=n_row, n_col=n_col),
        in_specs=[vmem()] * 6,
        out_specs=[vmem(), vmem()],
        out_shape=[
            jax.ShapeDtypeStruct((rows, LANES), jnp.float32),
            jax.ShapeDtypeStruct((n_row * n_col, 1, LANES), jnp.float32),
        ],
        scratch_shapes=[plane] * 6,
        compiler_params=params(12),
    )(sums, received, step_dir, image, from_right, from_left)


def neighbours(count):
    forward = [(i, i + 1) for i in range(count - 1)]
    return forward, [(j, i) for i, j in forward]


def step(residual, strip_weights, bin_weights, touched, image, precond):
    n_row = lax.axis_size(ROW)
    n_col = lax.axis_size(COL)
    n_x = lax.axis_size("col_0")
    n_z = lax.axis_size("col_1")
    angles = residual.shape[0]
    marks = touched[0]
    others = angles - X_FIRST
    far = back_project(
        far_products_kernel, residual, bin_weights, marks,
        ((n_z // 2, X_FIRST), (n_z // 2, X_FIRST), (n_x // 2, others), (n_x // 2, others)),
        n_x, n_z,
    )
    far, residual = lax.optimization_barrier((far, residual))
    flight = {}

    def send(name, pair):
        axis = "col_0" if name.endswith("x") else "col_1"
        n = lax.axis_size(axis)
        ring = [(i, (i + 1) % n) for i in range(n)]
        flight[name] = (
            lax.ppermute(pair[0], axis, ring),
            lax.ppermute(pair[1], axis, [(j, i) for i, j in ring]),
        )

    send("first_x", far[:2])
    send("first_z", far[2:])
    x_chunks, z_chunks = back_project(
        near_products_kernel, residual, bin_weights, marks,
        ((n_x, n_z, X_FIRST), (n_z, n_x, others)), n_x, n_z,
    )
    chunks = {"first_x": x_chunks, "first_z": z_chunks}
    waiting = []

    def flush(here):
        if waiting:
            name, pair = waiting.pop()
            pair, here = lax.optimization_barrier((pair, here))
            send(name, pair)
        return here

    def onward(name, step):
        here = flush(chunks[name])
        waiting.append((name, relay(here, *flight[name], step)))

    def turn(name, then, axis):
        here = flush(chunks[name])
        up, down, chunks[then] = collect(here, *flight[name], axis)
        waiting.append((then, (up, down)))

    onward("first_z", 3)
    onward("first_x", 1)
    onward("first_z", 2)
    onward("first_z", 1)
    turn("first_x", "then_z", "col_1")
    turn("first_z", "then_x", "col_0")
    onward("then_z", 3)
    onward("then_x", 1)
    onward("then_z", 2)
    onward("then_z", 1)
    groups = [flush(chunks["then_z"]), *flight["then_z"], chunks["then_x"], *flight["then_x"]]
    strip = strip_weights.T
    step_dir, row_slots = make_gradient(groups, strip, precond, image, n_row)
    received = lax.all_to_all(row_slots, ROW, 0, 0, tiled=True)
    leftward, rightward, sum_slots = make_edges(received, step_dir, image, n_row, n_col)
    later, earlier = neighbours(n_col)
    sums = lax.all_to_all(sum_slots, COL, 0, 0, tiled=True)
    from_right = lax.ppermute(leftward, COL, earlier)
    from_left = lax.ppermute(rightward, COL, later)
    updated, change_slots = denoise(
        sums, received, step_dir, image, from_right, from_left, n_row, n_col
    )
    changes = lax.all_to_all(change_slots, ROW_COL, 0, 0, tiled=True)
    cells = float(n_row * image.shape[0] * n_col * image.shape[1])
    return updated, jnp.sum(changes) / cells


def solution(mesh):
    split = Mesh(mesh.devices.reshape(4, 2, 4, 8), ("row_0", "row_1", "col_0", "col_1"))
    placed = (
        P(ROW, COL),
        P(ROW, None),
        P(ROW, COL, None),
        P(ROW, COL, None),
        P(ROW, COL),
        P(ROW, COL),
    )
    return jax.shard_map(
        step, mesh=split, in_specs=placed, out_specs=(P(ROW, COL), P()), check_vma=False
    )
```

```python
import functools

import jax
import jax.numpy as jnp
from jax import lax
from jax.experimental import pallas as pl
from jax.experimental.pallas import tpu as pltpu
from jax.sharding import Mesh
from jax.sharding import PartitionSpec as P


ITERS = 10
COL = ("col_0", "col_1")
ROW = ("row_0", "row_1")
ROW_COL = ("row_0", "row_1", "col_0", "col_1")

tv_weight = 0.25
dual_step = 0.125
radius = 0.25
epsilon = 1e-06

HALO = 16
X_FIRST = 128
LANES = 128
BASE = 8


def vmem():
    return pl.BlockSpec(memory_space=pltpu.VMEM)


def smem():
    return pl.BlockSpec(memory_space=pltpu.SMEM)


def params(mebibytes):
    return pltpu.CompilerParams(vmem_limit_bytes=mebibytes * 1024 * 1024)


def turned(axis, steps):
    return lax.rem(lax.axis_index(axis) + steps, lax.axis_size(axis))


def marked_products(marks, residual, weights, angles, tile, width):
    columns = pl.ds(pl.multiple_of(tile * LANES, width * LANES), width * LANES)
    product = jnp.dot(
        residual[slice(*angles)], weights[0, :, columns], preferred_element_type=jnp.float32
    )
    for t in range(width):
        yield t, product[:, t * LANES:(t + 1) * LANES] * marks[0, tile + t].astype(jnp.float32)


def far_products_kernel(marks, residual, weights, x_up, x_down, z_up, z_down, *, n_x, n_z):
    split = x_up.shape[1]
    x, z = turned("col_0", n_x // 2), turned("col_1", n_z // 2)
    width = n_z // 2
    for half, out in enumerate((x_up, x_down)):
        tile = x * n_z + half * width
        for t, value in marked_products(marks, residual, weights, (0, split), tile, width):
            out[t] = value
    for half, out in enumerate((z_up, z_down)):
        for k in range(n_x // 2):
            tile = (half * (n_x // 2) + k) * n_z + z
            for _, value in marked_products(marks, residual, weights, (split, None), tile, 1):
                out[k] = value


def near_products_kernel(marks, residual, weights, by_x, by_z, *, n_x, n_z):
    split = by_x.shape[2]
    width = n_z // 2
    for step in range(n_x):
        if step == n_x // 2:
            continue
        for z in range(0, n_z, width):
            tile = turned("col_0", step) * n_z + z
            for t, value in marked_products(marks, residual, weights, (0, split), tile, width):
                by_x[step, z + t] = value
    for x in range(n_x):
        for z in range(0, n_z, width):
            tile = x * n_z + z
            for t, value in marked_products(marks, residual, weights, (split, None), tile, width):
                steps = lax.rem(z + t + n_z - lax.axis_index("col_1"), n_z)
                by_z[steps, x] = value


def back_project(kernel, residual, weights, marks, shapes, n_x, n_z):
    return pl.pallas_call(
        functools.partial(kernel, n_x=n_x, n_z=n_z),
        in_specs=[smem(), vmem(), vmem()],
        out_specs=[vmem()] * len(shapes),
        out_shape=[jax.ShapeDtypeStruct(shape + (LANES,), jnp.float32) for shape in shapes],
        compiler_params=params(32),
    )(marks, residual, weights)


def relay_kernel(chunks, *refs, step):
    from_behind, *from_ahead, to_ahead, to_behind = refs
    ahead, behind = chunks.at[step], chunks.at[chunks.shape[0] - step]
    count = to_ahead.shape[0]
    brought = from_behind.shape[0]
    for k in range(count):
        value = ahead[k]
        to_ahead[k] = value + from_behind[k] if k < brought else value
        value = behind[k]
        here = k - (count - brought)
        to_behind[k] = value + from_ahead[0][here] if from_ahead and here >= 0 else value


def relay(chunks, brought, step):
    shape = jax.ShapeDtypeStruct(chunks.shape[1:], jnp.float32)
    return pl.pallas_call(
        functools.partial(relay_kernel, step=step),
        in_specs=[vmem()] * (1 + len(brought)),
        out_specs=[vmem()] * 2,
        out_shape=[shape, shape],
        compiler_params=params(8),
    )(chunks, *brought)


def collect_kernel(chunks, from_behind, from_ahead, far, out, *, axis):
    n = chunks.shape[1]
    half = far.shape[1]
    for step in range(n):
        k = turned(axis, step)
        total = chunks[0, k] + from_behind[k] + from_ahead[k]
        if step == n // 2:
            far[0], far[1] = total[:half], total[half:]
        else:
            out[step, 0], out[step, 1] = total[:half], total[half:]


def collect(chunks, from_behind, from_ahead, axis):
    _, n, angles, _ = chunks.shape
    far = jax.ShapeDtypeStruct((2, angles // 2, LANES), jnp.float32)
    return pl.pallas_call(
        functools.partial(collect_kernel, axis=axis),
        in_specs=[vmem()] * 3,
        out_specs=[vmem()] * 2,
        out_shape=[far, jax.ShapeDtypeStruct((n, 2, angles // 2, LANES), jnp.float32)],
        compiler_params=params(8),
    )(chunks, from_behind, from_ahead)


def exact_parts(value):
    high = value.astype(jnp.bfloat16)
    rest = value - high.astype(jnp.float32)
    middle = rest.astype(jnp.bfloat16)
    low = (rest - middle.astype(jnp.float32)).astype(jnp.bfloat16)
    return high, middle, low


def gradient_kernel(*refs, n_row):
    *groups, strip, precond, image, step_dir, slots = refs
    sums = []
    for k in range(0, len(groups), 3):
        chunks, from_behind, from_ahead = groups[k:k + 3]
        for half in range(2):
            sums.append(chunks[0, half] + from_behind[half] + from_ahead[half])
    summed = jnp.concatenate(sums, axis=0)
    gradient = None
    for piece in reversed(exact_parts(summed)):
        term = jnp.dot(strip[...], piece, preferred_element_type=jnp.float32)
        gradient = term if gradient is None else gradient + term
    value = precond[...] * gradient
    step_dir[...] = value
    rows = value.shape[0]
    squares = value * value
    partial = squares[0:8]
    for k in range(1, rows // 8):
        partial = partial + squares[8 * k:8 * k + 8]
    own = lax.axis_index(ROW)
    last = slice(rows - HALO, rows)
    for k in range(n_row):
        below = own < k
        slots[k, 0:HALO] = jnp.where(below, value[last], value[0:HALO])
        slots[k, HALO:2 * HALO] = jnp.where(below, image[last], image[0:HALO])
        slots[k, 2 * HALO:2 * HALO + 8] = partial


def make_gradient(groups, strip, precond, image, n_row):
    rows = strip.shape[0]
    return pl.pallas_call(
        functools.partial(gradient_kernel, n_row=n_row),
        in_specs=[vmem()] * (len(groups) + 3),
        out_specs=[vmem(), vmem()],
        out_shape=[
            jax.ShapeDtypeStruct((rows, LANES), jnp.float32),
            jax.ShapeDtypeStruct((n_row, 2 * HALO + 8, LANES), jnp.float32),
        ],
        compiler_params=params(8),
    )(*groups, strip, precond, image)


def edges_kernel(received, step_dir, image, leftward, rightward, slots, padded, *, n_row):
    own = lax.axis_index(ROW)
    rows = step_dir.shape[0]
    above = jnp.maximum(own - 1, 0)
    below = jnp.minimum(own + 1, n_row - 1)
    padded[rows + 2 * HALO:] = jnp.zeros((padded.shape[0] - rows - 2 * HALO, LANES), jnp.float32)
    for part, tile in enumerate((step_dir, image)):
        layers = slice(part * HALO, (part + 1) * HALO)
        padded[0:HALO] = received[above, layers]
        padded[HALO:HALO + rows] = tile[...]
        padded[HALO + rows:rows + 2 * HALO] = received[below, layers]
        for k in range(padded.shape[0] // LANES):
            here = slice(k * LANES, (k + 1) * LANES)
            block = padded[here].T
            leftward[layers, here] = block[0:HALO]
            rightward[layers, here] = block[LANES - HALO:]
    partial = received[0, 2 * HALO:2 * HALO + 8]
    for k in range(1, n_row):
        partial = partial + received[k, 2 * HALO:2 * HALO + 8]
    total = jnp.sum(partial, axis=0, keepdims=True)
    slots[...] = jnp.broadcast_to(total[None], slots.shape)


def make_edges(received, step_dir, image, n_row, n_col):
    rows = step_dir.shape[0]
    length = -(-(rows + 2 * HALO) // LANES) * LANES
    edge = jax.ShapeDtypeStruct((2 * HALO, length), jnp.float32)
    return pl.pallas_call(
        functools.partial(edges_kernel, n_row=n_row),
        in_specs=[vmem()] * 3,
        out_specs=[vmem(), vmem(), vmem()],
        out_shape=[edge, edge, jax.ShapeDtypeStruct((n_col, 1, LANES), jnp.float32)],
        scratch_shapes=[pltpu.VMEM((length, LANES), jnp.float32)],
        compiler_params=params(4),
    )(received, step_dir, image)


def denoise_kernel(
    sums, received, step_dir, image, from_right, from_left,
    updated, slots, scaled, down, right, potential, down_mask, right_mask,
    *, n_row, n_col,
):
    own_row, own_col = lax.axis_index(ROW), lax.axis_index(COL)
    rows = step_dir.shape[0]
    band = rows + 2 * HALO
    cells = float(n_row * rows * n_col * LANES)
    square_sum = jnp.sum(jnp.sum(sums[...], axis=0), axis=1, keepdims=True)
    spread = jnp.sqrt(square_sum / cells + epsilon)
    factor = jnp.minimum(1.0, radius / spread)

    zero = jnp.zeros((2, 8, LANES), jnp.float32)
    for plane in (scaled, down, right, potential):
        plane[:, 0:BASE] = zero
        plane[:, BASE + band:BASE + band + 8] = zero

    lane = lax.broadcasted_iota(jnp.int32, (8, LANES), 1)
    sub = lax.broadcasted_iota(jnp.int32, (8, LANES), 0)
    first_lane = lane == 0
    last_lane = lane == LANES - 1
    total_rows = n_row * rows
    total_cols = n_col * LANES
    columns = (
        own_col * LANES + lane,
        own_col * LANES + lane + jnp.where(lane < LANES // 2, LANES, -LANES),
    )
    column_in = [(c >= 0) & (c < total_cols) for c in columns]
    column_not_last = [(c >= 0) & (c < total_cols - 1) for c in columns]
    for at in range(BASE, BASE + band, 8):
        row = own_row * rows + (at - BASE - HALO) + sub
        row_in = (row >= 0) & (row < total_rows)
        row_not_last = (row >= 0) & (row < total_rows - 1)
        for t in range(2):
            down_mask[t, at:at + 8] = jnp.where(row_not_last & column_in[t], dual_step, 0.0)
            right_mask[t, at:at + 8] = jnp.where(row_in & column_not_last[t], dual_step, 0.0)
            down[t, at:at + 8] = zero[0]
            right[t, at:at + 8] = zero[0]

    def scale(direction, picture):
        return (picture - factor * direction) / tv_weight

    above = jnp.maximum(own_row - 1, 0)
    below = jnp.minimum(own_row + 1, n_row - 1)
    for there, at in ((above, BASE), (below, BASE + HALO + rows)):
        for k in range(0, HALO, 8):
            scaled[0, at + k:at + k + 8] = scale(
                received[there, k:k + 8], received[there, HALO + k:HALO + k + 8]
            )
    for at in range(0, rows, 8):
        scaled[0, BASE + HALO + at:BASE + HALO + at + 8] = scale(
            step_dir[at:at + 8], image[at:at + 8]
        )
    gap = jnp.zeros((LANES - 2 * HALO, LANES), jnp.float32)
    for k in range(from_right.shape[1] // LANES):
        here = slice(k * LANES, (k + 1) * LANES)
        edges = [
            scale(edge[0:HALO, here], edge[HALO:2 * HALO, here]) for edge in (from_right, from_left)
        ]
        block = jnp.concatenate([edges[0], gap, edges[1]], axis=0).T
        count = min(LANES, band - k * LANES)
        scaled[1, BASE + k * LANES:BASE + k * LANES + count] = block[0:count]

    def right_divergence(at, t):
        mine = right[t, at:at + 8]
        rolled = pltpu.roll(mine, 1, 1)
        across = pltpu.roll(right[1 - t, at:at + 8], 1, 1)
        return mine - jnp.where(first_lane, across, rolled)

    def turn(_, carry):
        for at in range(BASE, BASE + band, 8):
            rolled = [pltpu.roll(right[t, at:at + 8], 1, 1) for t in range(2)]
            for t in range(2):
                beside = jnp.where(first_lane, rolled[1 - t], rolled[t])
                potential[t, at:at + 8] = (
                    (down[t, at:at + 8] - down[t, at - 1:at + 7])
                    + (right[t, at:at + 8] - beside)
                    - scaled[t, at:at + 8]
                )
        for at in range(BASE, BASE + band, 8):
            here = [potential[t, at:at + 8] for t in range(2)]
            rolled = [pltpu.roll(here[t], LANES - 1, 1) for t in range(2)]
            for t in range(2):
                beside = jnp.where(last_lane, rolled[1 - t], rolled[t])
                step_down = (potential[t, at + 1:at + 9] - here[t]) * down_mask[t, at:at + 8]
                step_right = (beside - here[t]) * right_mask[t, at:at + 8]
                square = step_down * step_down + step_right * step_right
                size = square * lax.rsqrt(jnp.maximum(square, 1e-36))
                inverse = 1.0 / (1.0 + size)
                down[t, at:at + 8] = (down[t, at:at + 8] + step_down) * inverse
                right[t, at:at + 8] = (right[t, at:at + 8] + step_right) * inverse
        return carry

    lax.fori_loop(0, ITERS, turn, 0)

    change_sum = jnp.zeros((8, LANES), jnp.float32)
    for at in range(BASE + HALO, BASE + HALO + rows, 8):
        inner = at - BASE - HALO
        picture = image[inner:inner + 8]
        source = picture - factor * step_dir[inner:inner + 8]
        divergence = (down[0, at:at + 8] - down[0, at - 1:at + 7]) + right_divergence(at, 0)
        result = source - tv_weight * divergence
        updated[inner:inner + 8] = result
        change = result - picture
        change_sum = change_sum + change * change
    total = jnp.sum(change_sum, axis=0, keepdims=True)
    slots[...] = jnp.broadcast_to(total[None], slots.shape)


def denoise(sums, received, step_dir, image, from_right, from_left, n_row, n_col):
    rows = step_dir.shape[0]
    plane = pltpu.VMEM((2, BASE + rows + 2 * HALO + 8, LANES), jnp.float32)
    return pl.pallas_call(
        functools.partial(denoise_kernel, n_row=n_row, n_col=n_col),
        in_specs=[vmem()] * 6,
        out_specs=[vmem(), vmem()],
        out_shape=[
            jax.ShapeDtypeStruct((rows, LANES), jnp.float32),
            jax.ShapeDtypeStruct((n_row * n_col, 1, LANES), jnp.float32),
        ],
        scratch_shapes=[plane] * 6,
        compiler_params=params(12),
    )(sums, received, step_dir, image, from_right, from_left)


def neighbours(count):
    forward = [(i, i + 1) for i in range(count - 1)]
    return forward, [(j, i) for i, j in forward]


def step(residual, strip_weights, bin_weights, touched, image, precond):
    n_row = lax.axis_size(ROW)
    n_col = lax.axis_size(COL)
    n_x = lax.axis_size("col_0")
    n_z = lax.axis_size("col_1")
    angles = residual.shape[0]
    marks = touched[0]
    others = angles - X_FIRST
    far = back_project(
        far_products_kernel, residual, bin_weights, marks,
        ((n_z // 2, X_FIRST), (n_z // 2, X_FIRST), (n_x // 2, others), (n_x // 2, others)),
        n_x, n_z,
    )
    far, residual = lax.optimization_barrier((far, residual))
    flight = {}

    def send(name, pair):
        axis = "col_0" if name.endswith("x") else "col_1"
        n = lax.axis_size(axis)
        ring = [(i, (i + 1) % n) for i in range(n)]
        ways = (ring, [(j, i) for i, j in ring])
        flight[name] = [lax.ppermute(part, axis, way) for part, way in zip(pair, ways)]

    send("first_x", far[:2])
    send("first_z", far[2:])
    x_chunks, z_chunks = back_project(
        near_products_kernel, residual, bin_weights, marks,
        ((n_x, n_z, X_FIRST), (n_z, n_x, others)), n_x, n_z,
    )
    chunks = {"first_x": x_chunks, "first_z": z_chunks}
    waiting = []

    def flush(here):
        if waiting:
            name, pair = waiting.pop()
            pair, here = lax.optimization_barrier((pair, here))
            send(name, pair)
        return here

    def onward(name, step):
        here = flush(chunks[name])
        waiting.append((name, relay(here, flight[name], step)))

    def turn(name, then, axis):
        here = flush(chunks[name])
        far, chunks[then] = collect(here, *flight[name], axis)
        waiting.append((then, (far,)))

    onward("first_z", 3)
    onward("first_x", 1)
    onward("first_z", 2)
    turn("first_x", "then_z", "col_1")
    onward("first_z", 1)
    turn("first_z", "then_x", "col_0")
    onward("then_z", 3)
    onward("then_x", 1)
    onward("then_z", 2)
    onward("then_z", 1)
    groups = [flush(chunks["then_z"]), *flight["then_z"], chunks["then_x"], *flight["then_x"]]
    strip = strip_weights.T
    step_dir, row_slots = make_gradient(groups, strip, precond, image, n_row)
    received = lax.all_to_all(row_slots, ROW, 0, 0, tiled=True)
    leftward, rightward, sum_slots = make_edges(received, step_dir, image, n_row, n_col)
    later, earlier = neighbours(n_col)
    sums = lax.all_to_all(sum_slots, COL, 0, 0, tiled=True)
    from_right = lax.ppermute(leftward, COL, earlier)
    from_left = lax.ppermute(rightward, COL, later)
    updated, change_slots = denoise(
        sums, received, step_dir, image, from_right, from_left, n_row, n_col
    )
    changes = lax.all_to_all(change_slots, ROW_COL, 0, 0, tiled=True)
    cells = float(n_row * image.shape[0] * n_col * image.shape[1])
    return updated, jnp.sum(changes) / cells


def solution(mesh):
    split = Mesh(mesh.devices.reshape(4, 2, 4, 8), ("row_0", "row_1", "col_0", "col_1"))
    placed = (
        P(ROW, COL),
        P(ROW, None),
        P(ROW, COL, None),
        P(ROW, COL, None),
        P(ROW, COL),
        P(ROW, COL),
    )
    return jax.shard_map(
        step, mesh=split, in_specs=placed, out_specs=(P(ROW, COL), P()), check_vma=False
    )
```
